32 devices in a mesh: parts: 2 (over y), dp: 4 (over x, core), tp: 4 (over z).
Axes of the slice: x: 2, y: 2, z: 4, core: 2. Of those that a mesh axis runs over, the one named last changes fastest.
Arguments:
- hidden: bfloat16 [32, 128, 8192], P(('parts', 'dp'), 'tp'), parts along dimension 0, may hold values from -6 to 6
- norm_gain: bfloat16 [8192], replicated, may hold values from 0.099609375 to 1.8984375
- w_query: bfloat16 [8192, 4096], P(None, 'tp'), may hold values from -0.0625 to 0.0625
- w_keyval: bfloat16 [8192, 1024], P(None, 'tp'), may hold values from -0.0625 to 0.0625
- w_out: bfloat16 [4096, 8192], P('tp'), may hold values from -0.5 to 0.5
- kv_cache: bfloat16 [1024, 16, 32, 256], P(('parts', 'dp'), 'tp'), parts along dimension 0, may hold values from -600 to 600
- page_table: int32 [32, 32], P(('parts', 'dp')), parts along dimension 0, may hold values from 0 to 127, as said below
- prefix_len: int32 [32], P(('parts', 'dp')), parts along dimension 0, may hold values from 0 to 4096, as said below
- live_rows: int32 [32], P(('parts', 'dp')), parts along dimension 0, may hold values from 1 to 128
- plan: int32 [32], P(('parts', 'dp')), parts along dimension 0, may hold values from 0 to 3, as said below
Outputs:
- result: bfloat16 [32, 128, 8192], P(('parts', 'dp'), 'tp'), parts along dimension 0
- new_kv: bfloat16 [32, 128, 1024], P(('parts', 'dp'), None, 'tp'), parts along dimension 0
The draws below stay inside these ranges and needn't reach their ends.
There are 2 independent parts, one for each index of `parts`. The reference program is written for one: setup_inputs(seed, part) draws one part's arguments, and reference() takes and returns one part's arrays. A program takes and returns all parts, laid end to end along the dimension named above; an argument that names none is the same for every part. Nothing has to cross between parts.
Inputs may be any that keep to these rules, and one draw needn't show every extreme that they name: `page_table`: the 32 pages listed for a stretch belong to its own group, and no page is listed twice within a group. `prefix_len`: a multiple of 128; within a group it never grows with the slot number. `plan`: the 4 stretches of one group go to different groups, and every group receives exactly one stretch of each slot number.
All inputs are finite; a program needn't handle non-finite values.
Results may differ from the reference program's by a relative error of at most 0.02.
The reference program's roundings to bfloat16 on the way count: a program that leaves them out, or rounds other values in their place, can miss the bound.
Values may be sent and summed in bfloat16 or wider, within the bound.
A program may use at most 128 MiB of HBM per device.

```python
import math
import jax
import jax.numpy as jnp
from jax import lax

D = 8192
HEADS = 32
KV_HEADS = 4
HEAD_DIM = 128
SPLIT = 4
BLOCK = 128
MAX_PAGES = 32
OWN = 4
STRETCH = 128
GROUPS = 4
STRETCHES = 16
POOL = 128
N_TP = 4


def draw_kv_cache(key, part):
    shape = (GROUPS * POOL, KV_HEADS * SPLIT, BLOCK // SPLIT, 2 * HEAD_DIM)
    first_key = jax.random.fold_in(jax.random.fold_in(key, 71), 0)
    values = jnp.clip(jax.random.normal(first_key, shape, jnp.float32), -6.0, 6.0)
    return values.astype(jnp.bfloat16)


def draw_page_table(key, part):
    group_keys = jax.random.split(jax.random.fold_in(key, 11), GROUPS)
    orders = jax.vmap(lambda single: jax.random.permutation(single, POOL))(group_keys)
    return orders.reshape(GROUPS * OWN, MAX_PAGES).astype(jnp.int32)


def draw_prefix_len(key, part):
    first_key, second_key, third_key = jax.random.split(jax.random.fold_in(key, 23), 3)
    levels = jax.random.randint(first_key, (GROUPS, 1), 1, 5)
    raw_pages = jax.random.randint(second_key, (GROUPS, OWN), 0, MAX_PAGES + 1)
    page_counts = raw_pages * levels // 4
    heavy = jax.random.randint(third_key, (), 0, GROUPS)
    corner = (jnp.arange(GROUPS)[:, None] == heavy) & (jnp.arange(OWN)[None, :] == 0)
    page_counts = jnp.where(corner, MAX_PAGES, page_counts)
    page_counts = -jnp.sort(-page_counts, axis=1)
    return (page_counts * BLOCK).reshape(GROUPS * OWN).astype(jnp.int32)


def draw_live_rows(key, part):
    first_key, second_key, third_key = jax.random.split(jax.random.fold_in(key, 37), 3)
    whole = jax.random.randint(first_key, (STRETCHES,), 0, 2)
    shorter = jax.random.randint(second_key, (STRETCHES,), 1, STRETCH + 1)
    counts = jnp.where(whole == 1, STRETCH, shorter)
    forced = jax.random.randint(third_key, (), 0, STRETCHES)
    counts = jnp.where(jnp.arange(STRETCHES) == forced, STRETCH, counts)
    return counts.astype(jnp.int32)


def draw_plan(key, part):
    lengths = draw_prefix_len(key, part).reshape(GROUPS, OWN)
    loads = jnp.sum(lengths // BLOCK, axis=1).astype(jnp.int32)
    group_ids = jnp.arange(GROUPS, dtype=jnp.int32)
    scores = loads * GROUPS + group_ids
    order = jnp.argsort(-scores).astype(jnp.int32)
    ranking = jnp.zeros((GROUPS,), jnp.int32).at[order].set(group_ids)
    slot_ids = jnp.arange(OWN, dtype=jnp.int32)
    target_rank = (GROUPS - 1 - ranking[:, None] + slot_ids[None, :]) % GROUPS
    targets = order[target_rank]
    return targets.reshape(STRETCHES).astype(jnp.int32)


def shard_levels(key, shape, cuts, least, high):
    level = 1.0
    for position, blocks in cuts:
        heights = jax.random.uniform(jax.random.fold_in(jax.random.fold_in(key, 6), position), (blocks,), jnp.float32, least / len(cuts), high / len(cuts))
        level = level * jnp.repeat(jnp.exp(heights), shape[position] // blocks).reshape((-1,) + (1,) * (len(shape) - 1 - position))
    return level


def bell_draw(rng, extent, width, reach, cuts=(), kind=jnp.bfloat16):
    array = width * jax.random.normal(rng, extent, jnp.float32)
    if cuts:
        array = array * shard_levels(rng, extent, cuts, -0.22, 0.18)
    return jnp.clip(array, -reach, reach).astype(kind)


def setup_inputs(seed: int = 0, part: int = 0) -> dict:
    seeds = jax.random.split(jax.random.key(seed), 11)
    part_splits = jax.random.split(jax.random.fold_in(seeds[10], part), 11)
    hidden = bell_draw(part_splits[0], (STRETCHES, STRETCH, D), 1.0, 6.0, ((0, 4), (1, 4)))
    norm_gain = jnp.clip(1.0 + 0.18 * jax.random.normal(seeds[1], (D,), jnp.float32), 0.099609375, 1.8984375).astype(jnp.bfloat16)
    w_query = bell_draw(seeds[2], (D, HEADS * HEAD_DIM), D ** -0.5, 0.0625, ((1, 4),))
    w_keyval = bell_draw(seeds[3], (D, KV_HEADS * 2 * HEAD_DIM), D ** -0.5, 0.0625, ((1, 4),))
    w_out = bell_draw(seeds[4], (HEADS * HEAD_DIM, D), HEAD_DIM ** -0.5, 0.5, ((0, 4),))
    kv_cache = draw_kv_cache(jax.random.fold_in(jax.random.fold_in(seeds[10], part), 71), part)
    page_table = draw_page_table(jax.random.fold_in(jax.random.fold_in(seeds[10], part), 71), part)
    prefix_len = draw_prefix_len(jax.random.fold_in(jax.random.fold_in(seeds[10], part), 71), part)
    live_rows = draw_live_rows(jax.random.fold_in(jax.random.fold_in(seeds[10], part), 71), part)
    plan = draw_plan(jax.random.fold_in(jax.random.fold_in(seeds[10], part), 71), part)
    return dict(hidden=hidden, norm_gain=norm_gain, w_query=w_query, w_keyval=w_keyval, w_out=w_out, kv_cache=kv_cache, page_table=page_table, prefix_len=prefix_len, live_rows=live_rows, plan=plan)


EPSILON = 1e-05
ROPE_BASE = 500000.0
MASKED = -1e+30

def rotate(values, positions):
    half_width = values.shape[-1] // 2
    frequency = ROPE_BASE ** (-jnp.arange(half_width, dtype=jnp.float32) / half_width)
    angles = positions.astype(jnp.float32)[..., None] * frequency
    cosine = jnp.cos(angles)[..., None, :]
    sine_values = jnp.sin(angles)[..., None, :]
    front_half = values[..., :half_width]
    back_half = values[..., half_width:]
    return jnp.concatenate([front_half * cosine - back_half * sine_values, back_half * cosine + front_half * sine_values], axis=-1)

def one_stretch(stretch_id, hidden, norm_gain, w_query, w_keyval, out_wide, kv_cache, page_table, prefix_len, live_rows):
    stretch_rows = hidden[stretch_id]
    owner_group = stretch_id // OWN
    widened = stretch_rows.astype(jnp.float32)
    normed = (widened * lax.rsqrt(lax.optimization_barrier(jnp.mean(widened * widened, axis=-1, keepdims=True)) + EPSILON) * norm_gain.astype(jnp.float32)).astype(jnp.bfloat16)
    start_pos = prefix_len[stretch_id]
    positions = start_pos + jnp.arange(STRETCH, dtype=jnp.int32)
    queries = rotate(jnp.dot(normed, w_query, preferred_element_type=jnp.float32).reshape(STRETCH, HEADS, HEAD_DIM), positions).astype(jnp.bfloat16)
    pairs = jnp.dot(normed, w_keyval, preferred_element_type=jnp.float32).astype(jnp.bfloat16).reshape(STRETCH, KV_HEADS, 2 * HEAD_DIM)
    rotated = rotate(pairs[..., :HEAD_DIM].astype(jnp.float32), positions)
    row_index = jnp.arange(STRETCH, dtype=jnp.int32)
    live_mask = row_index < live_rows[stretch_id]
    new_pairs = (jnp.concatenate([rotated, pairs[..., HEAD_DIM:].astype(jnp.float32)], axis=-1) * live_mask[:, None, None].astype(jnp.float32)).astype(jnp.bfloat16)
    page_ids = (owner_group * POOL + page_table[stretch_id]).astype(jnp.int32)
    stored = kv_cache[page_ids].reshape(MAX_PAGES, KV_HEADS, BLOCK, 2 * HEAD_DIM)
    stored = jnp.transpose(stored, (1, 0, 2, 3)).reshape(KV_HEADS, MAX_PAGES * BLOCK, 2 * HEAD_DIM)
    every_pair = jnp.concatenate([stored, jnp.transpose(new_pairs, (1, 0, 2))], axis=1).astype(jnp.float32)
    grouped = queries.astype(jnp.float32).reshape(STRETCH, KV_HEADS, HEADS // KV_HEADS, HEAD_DIM)
    scores = jnp.einsum('cgqd,gtd->gqct', grouped, every_pair[..., :HEAD_DIM]) * (1.0 / math.sqrt(HEAD_DIM))
    key_place = jnp.arange(MAX_PAGES * BLOCK, dtype=jnp.int32)
    prefix_mask = jnp.broadcast_to(key_place[None, :] < start_pos, (STRETCH, MAX_PAGES * BLOCK))
    own_mask = (row_index[None, :] <= row_index[:, None]) & live_mask[None, :]
    full_mask = jnp.concatenate([prefix_mask, own_mask], axis=1)
    scores = jnp.where(full_mask[None, None], scores, MASKED)
    peak = lax.optimization_barrier(jnp.max(scores, axis=-1, keepdims=True))
    exps = jnp.exp(scores - peak)
    weights = (exps / lax.optimization_barrier(jnp.sum(exps, axis=-1, keepdims=True))).astype(jnp.bfloat16)
    attended = jnp.einsum('gqct,gtd->cgqd', weights.astype(jnp.float32), every_pair[..., HEAD_DIM:]).astype(jnp.bfloat16)
    group_width = HEADS * HEAD_DIM // N_TP
    attended = attended.astype(jnp.float32).reshape(STRETCH, N_TP, group_width)
    partial_value = jnp.einsum('cnk,nkd->ncd', attended, out_wide.reshape(N_TP, group_width, D)).astype(jnp.bfloat16)
    branch = lax.optimization_barrier(jnp.sum(partial_value.astype(jnp.float32), axis=0))
    branch = jnp.where(live_mask[:, None], branch, jnp.zeros_like(branch)).astype(jnp.bfloat16)
    return (branch, new_pairs.reshape(STRETCH, KV_HEADS * 2 * HEAD_DIM))

def reference(hidden, norm_gain, w_query, w_keyval, w_out, kv_cache, page_table, prefix_len, live_rows, plan):
    out_wide = w_out.astype(jnp.float32)

    def per_stretch(stretch_id):
        return one_stretch(stretch_id, hidden, norm_gain, w_query, w_keyval, out_wide, kv_cache, page_table, prefix_len, live_rows)
    branches, new_kv = lax.map(per_stretch, jnp.arange(STRETCHES, dtype=jnp.int32))
    places = (plan * OWN + jnp.arange(STRETCHES, dtype=jnp.int32) % OWN).astype(jnp.int32)
    result = jnp.zeros_like(branches).at[places].set(branches)
    return (result, new_kv)
```

```python
import math

import jax
import jax.numpy as jnp
from jax import lax
from jax.sharding import PartitionSpec as P

KV_HEADS = 4
HEAD_DIM = 128
BLOCK = 128
MAX_PAGES = 32


EPSILON = 1e-05
ROPE_BASE = 500000.0
MASKED = -1e30


def from_partner(value, axis, distance):
    mask = 2**distance
    pairs = [(source, source ^ mask) for source in range(lax.axis_size(axis))]
    return lax.ppermute(value, axis, pairs)


def rotate(values, positions):
    half_width = values.shape[-1] // 2
    frequency = ROPE_BASE ** (-jnp.arange(half_width, dtype=jnp.float32) / half_width)
    angles = positions.astype(jnp.float32)[..., None] * frequency
    cosine = jnp.cos(angles)[..., None, :]
    sine_values = jnp.sin(angles)[..., None, :]
    front_half = values[..., :half_width]
    back_half = values[..., half_width:]
    return jnp.concatenate(
        [
            front_half * cosine - back_half * sine_values,
            back_half * cosine + front_half * sine_values,
        ],
        axis=-1,
    )


def attend_one(inputs):
    queries, head_pairs, prefix, start, count = inputs
    head_width = queries.shape[-1]
    scaling = 1.0 / math.sqrt(head_width)
    row_count = queries.shape[0]
    row_index = jnp.arange(row_count, dtype=jnp.int32)
    own_mask = (row_index[None, :] <= row_index[:, None]) & (row_index[None, :] < count)
    own_scores = (
        jnp.einsum(
            "chd,jd->hcj", queries, head_pairs[:, :head_width], preferred_element_type=jnp.float32
        )
        * scaling
    )
    own_scores = jnp.where(own_mask[None], own_scores, MASKED)
    span_pages = max(1, min(MAX_PAGES, 512 // BLOCK))
    key_span = span_pages * BLOCK
    block_count = (start + key_span - 1) // key_span

    def block_scores(block_id):
        key_block = lax.dynamic_slice_in_dim(prefix, block_id * key_span, key_span, 0)
        scores = (
            jnp.einsum(
                "chd,td->hct",
                queries,
                key_block[:, :head_width],
                preferred_element_type=jnp.float32,
            )
            * scaling
        )
        key_place = block_id * key_span + jnp.arange(key_span, dtype=jnp.int32)
        key_mask = key_place < start
        return (jnp.where(key_mask[None, None, :], scores, MASKED), key_block)

    running_max = jnp.max(own_scores, axis=-1)
    running_sum = jnp.sum(jnp.exp(own_scores - running_max[..., None]), axis=-1)

    def first_pass(block_id, state_pair):
        old_max, old_sum = state_pair
        scores, key_block = block_scores(block_id)
        raised_max = jnp.maximum(old_max, jnp.max(scores, axis=-1))
        new_sum = old_sum * jnp.exp(old_max - raised_max) + jnp.sum(
            jnp.exp(scores - raised_max[..., None]), axis=-1
        )
        return (raised_max, new_sum)

    running_max, running_sum = lax.fori_loop(0, block_count, first_pass, (running_max, running_sum))

    def normalize(scores):
        return (jnp.exp(scores - running_max[..., None]) / running_sum[..., None]).astype(
            jnp.bfloat16
        )

    attended = jnp.einsum(
        "hcj,jd->chd",
        normalize(own_scores),
        head_pairs[:, head_width:],
        preferred_element_type=jnp.float32,
    )

    def second_pass(block_id, gathered_sum):
        scores, key_block = block_scores(block_id)
        return gathered_sum + jnp.einsum(
            "hct,td->chd",
            normalize(scores),
            key_block[:, head_width:],
            preferred_element_type=jnp.float32,
        )

    attended = lax.fori_loop(0, block_count, second_pass, attended)
    return attended.astype(jnp.bfloat16)


def attend(queries, head_pairs, prefix, starts, counts):
    return lax.map(attend_one, (queries, head_pairs, prefix, starts, counts))


def layer(stretch_rows, stretch_pages, starts, counts, norm_gain, w_query, w_keyval, w_out):
    tensor_size = lax.axis_size("tp")
    tensor_rank = lax.axis_index("tp")
    widened = stretch_rows.astype(jnp.float32)
    normed = (
        widened
        * lax.rsqrt(jnp.mean(widened * widened, axis=-1, keepdims=True) + EPSILON)
        * norm_gain.astype(jnp.float32)
    ).astype(jnp.bfloat16)
    query_width = w_query.shape[1]
    portion = lax.all_gather(normed, "tp", axis=1, tiled=True)
    query_part = jnp.einsum("ocd,dk->ock", portion, w_query, preferred_element_type=jnp.float32)
    pair_part = jnp.einsum("ocd,dk->ock", portion, w_keyval, preferred_element_type=jnp.float32)
    projected = jnp.concatenate([query_part, pair_part], axis=-1)
    holding = projected.shape[0]
    length = projected.shape[1]
    head_width = HEAD_DIM
    positions = starts[:, None] + jnp.arange(length, dtype=jnp.int32)[None, :]
    queries = rotate(
        projected[..., :query_width].reshape(
            holding, length, query_width // head_width, head_width
        ),
        positions,
    ).astype(jnp.bfloat16)
    pair_piece = projected[..., query_width:].astype(jnp.bfloat16)
    sharers = tensor_size // KV_HEADS
    levels = sharers.bit_length() - 1
    sharer_rank = tensor_rank % sharers
    page_piece = stretch_pages
    for level_bit in range(levels):
        their_pairs, their_pages = from_partner((pair_piece, page_piece), "tp", level_bit)
        upper_half = tensor_rank // (1 << level_bit) % 2 == 1
        pair_piece = jnp.where(
            upper_half,
            jnp.concatenate([their_pairs, pair_piece], axis=-1),
            jnp.concatenate([pair_piece, their_pairs], axis=-1),
        )
        page_piece = jnp.where(
            upper_half,
            jnp.concatenate([their_pages, page_piece], axis=2),
            jnp.concatenate([page_piece, their_pages], axis=2),
        )
    live_mask = jnp.arange(length, dtype=jnp.int32)[None, :] < counts[:, None]
    rotated_keys = rotate(
        pair_piece[..., :head_width].astype(jnp.float32)[:, :, None, :], positions
    )[:, :, 0, :]
    head_pairs = (
        jnp.concatenate([rotated_keys, pair_piece[..., head_width:].astype(jnp.float32)], axis=-1)
        * live_mask[..., None].astype(jnp.float32)
    ).astype(jnp.bfloat16)
    piece_width = 2 * head_width // sharers
    columns = lax.dynamic_slice_in_dim(head_pairs, sharer_rank * piece_width, piece_width, 2)
    prefix = page_piece.reshape(holding, -1, 2 * head_width)
    attended = attend(queries, head_pairs, prefix, starts, counts)
    partial_value = jnp.einsum(
        "ock,kd->ocd",
        attended.reshape(holding, length, -1),
        w_out,
        preferred_element_type=jnp.float32,
    )
    summed = lax.psum_scatter(
        partial_value.astype(jnp.bfloat16), "tp", scatter_dimension=1, tiled=True
    ).astype(jnp.float32)
    share_rows = summed.shape[1]
    row_ids = tensor_rank * share_rows + jnp.arange(share_rows, dtype=jnp.int32)
    keep_rows = row_ids[None, :] < counts[:, None]
    result = jnp.where(keep_rows[..., None], summed, jnp.zeros_like(summed)).astype(jnp.bfloat16)
    return (result, columns)


def per_device_general(
    hidden, norm_gain, w_query, w_keyval, w_out, kv_cache, page_table, prefix_len, live_rows, plan
):
    groups = lax.axis_size("dp")
    holding = hidden.shape[0]
    slot_ids = jnp.arange(holding, dtype=jnp.int32)
    gathered_pages = kv_cache[page_table]
    target = jnp.arange(groups, dtype=jnp.int32)
    matches = plan[None, :] == target[:, None]
    present = jnp.any(matches, axis=1)
    chosen = jnp.argmax(matches, axis=1)
    labels = jnp.where(present, chosen, -1)
    local_rows, new_kv = layer(
        hidden, gathered_pages, prefix_len, live_rows, norm_gain, w_query, w_keyval, w_out
    )
    outgoing = jnp.where(
        present[:, None, None], local_rows[chosen], jnp.zeros((), local_rows.dtype)
    )
    arrived, labels_arrived = (
        lax.all_to_all(outgoing, "dp", split_axis=0, concat_axis=0, tiled=True),
        lax.all_to_all(labels, "dp", split_axis=0, concat_axis=0, tiled=True),
    )
    source = jnp.argmax(labels_arrived[None, :] == slot_ids[:, None], axis=1)
    result = arrived[source]
    return (result, new_kv)


def gather_rows(rows, gate):
    size = lax.axis_size("tp")
    up = [(source, source + 1) for source in range(size - 1)]
    down = [(source + 1, source) for source in range(size - 1)]
    if gate is not None:
        rows, _ = lax.optimization_barrier((rows, gate))
    risen = [rows]
    fallen = [rows]
    for _ in range(size - 1):
        risen.append(lax.ppermute(risen[-1], "tp", up))
        fallen.append(lax.ppermute(fallen[-1], "tp", down))
    rank = lax.axis_index("tp")
    pieces = [rows]
    for distance in range(1, size):
        pieces.append(jnp.where(rank >= distance, risen[distance], fallen[size - distance]))
    return jnp.concatenate(pieces, axis=0), (risen[1], fallen[1])


def project(portion, weight):
    return jnp.dot(portion, weight, preferred_element_type=jnp.float32)


def turn(values, share):
    size = lax.axis_size("tp")
    rank = lax.axis_index("tp")
    pieces = values.reshape(size, share, -1)
    places = (rank - jnp.arange(size, dtype=jnp.int32)) % size
    return pieces[places].reshape(size * share, -1)


def per_device(
    hidden, norm_gain, w_query, w_keyval, w_out, kv_cache, page_table, prefix_len, live_rows, plan
):
    groups = lax.axis_size("dp")
    size = lax.axis_size("tp")
    holding, share, _ = hidden.shape
    if groups != holding or groups & (groups - 1) or size != KV_HEADS:
        return per_device_general(
            hidden, norm_gain, w_query, w_keyval, w_out, kv_cache, page_table, prefix_len,
            live_rows, plan,
        )
    group = lax.axis_index("dp")
    rank = lax.axis_index("tp")
    length = share * size
    heads = w_query.shape[1] // HEAD_DIM
    gain = norm_gain.astype(jnp.float32)
    result = jnp.zeros_like(hidden)
    new_kv = jnp.zeros((holding, length, w_keyval.shape[1]), jnp.bfloat16)
    gate = None
    for offset in list(range(groups // 2, groups)) + list(range(groups // 2 - 1, -1, -1)):
        slot = jnp.argmax(plan == (group ^ offset)).astype(jnp.int32)
        start = prefix_len[slot]
        count = live_rows[slot]
        widened = hidden[slot].astype(jnp.float32)
        normed = (
            widened
            * lax.rsqrt(jnp.mean(widened * widened, axis=-1, keepdims=True) + EPSILON)
            * gain
        ).astype(jnp.bfloat16)
        if True:
            if gate is not None:
                normed, _ = lax.optimization_barrier((normed, gate))
            portion = lax.all_gather(normed, "tp", axis=0, tiled=True)
            gate = None
            order = lambda values: values
        else:
            portion, gate = gather_rows(normed, gate)
            order = lambda values: turn(values, share)
        positions = start + jnp.arange(length, dtype=jnp.int32)
        queries = rotate(
            order(project(portion, w_query)).reshape(length, heads, HEAD_DIM), positions
        ).astype(jnp.bfloat16)
        pairs = order(project(portion, w_keyval).astype(jnp.bfloat16))
        live_mask = jnp.arange(length, dtype=jnp.int32) < count
        rotated_keys = rotate(pairs[:, None, :HEAD_DIM].astype(jnp.float32), positions)[:, 0, :]
        head_pairs = (
            jnp.concatenate([rotated_keys, pairs[:, HEAD_DIM:].astype(jnp.float32)], axis=-1)
            * live_mask[:, None].astype(jnp.float32)
        ).astype(jnp.bfloat16)
        new_kv = lax.dynamic_update_slice_in_dim(new_kv, head_pairs[None], slot, 0)
        prefix = kv_cache[page_table[slot]].reshape(-1, 2 * HEAD_DIM)
        attended = attend_one((queries, head_pairs, prefix, start, count))
        partial_value = project(attended.reshape(length, -1), w_out).astype(jnp.bfloat16)
        summed = lax.psum_scatter(partial_value, "tp", scatter_dimension=0, tiled=True)
        row_ids = rank * share + jnp.arange(share, dtype=jnp.int32)
        branch = jnp.where((row_ids < count)[:, None], summed, jnp.zeros_like(summed))
        if offset:
            partners = [(source, source ^ offset) for source in range(groups)]
            branch = lax.ppermute(branch, "dp", partners)
            slot = lax.ppermute(slot[None], "dp", partners)[0]
        result = lax.dynamic_update_slice_in_dim(result, branch[None], slot, 0)
    return (result, new_kv)


def solution(mesh):
    in_specs = (
        P(("parts", "dp"), "tp", None),
        P(),
        P(None, "tp"),
        P(None, "tp"),
        P("tp", None),
        P(("parts", "dp"), "tp", None, None),
        P(("parts", "dp"), None),
        P(("parts", "dp")),
        P(("parts", "dp")),
        P(("parts", "dp")),
    )
    out_specs = (P(("parts", "dp"), "tp", None), P(("parts", "dp"), None, "tp"))
    return jax.shard_map(
        per_device, mesh=mesh, in_specs=in_specs, out_specs=out_specs, check_vma=False
    )
```
